32 devices in a mesh: dp: 4 (over y, z), tp: 8 (over x, core).
Axes of the slice: x: 4, y: 2, z: 2, core: 2. Of those that a mesh axis runs over, the one named last changes fastest.
The devices are a block of a 4x4x8 slice.
Arguments:
- hidden: bfloat16 [8, 512, 5120], P('dp', 'tp'), parts along dimension 0
- vision: bfloat16 [8, 2048, 5120], P('dp', 'tp'), parts along dimension 0
- positions: int32 [8, 512], P('dp', 'tp'), parts along dimension 0
- tile_mask: int32 [8, 512, 4], P('dp', 'tp'), parts along dimension 0
- ln1_a: bfloat16 [5120], replicated
- wq_a: bfloat16 [5120, 4096], P(None, 'tp')
- wk_a: bfloat16 [5120, 1024], P(None, 'tp')
- wv_a: bfloat16 [5120, 1024], P(None, 'tp')
- wo_a: bfloat16 [4096, 5120], P('tp')
- ln2_a: bfloat16 [5120], replicated
- wg_a: bfloat16 [5120, 14336], P(None, 'tp')
- wu_a: bfloat16 [5120, 14336], P(None, 'tp')
- wd_a: bfloat16 [14336, 5120], P('tp')
- ln1_b: bfloat16 [5120], replicated
- wq_b: bfloat16 [5120, 4096], P(None, 'tp')
- q_norm: bfloat16 [128], replicated
- wk_b: bfloat16 [5120, 1024], P(None, 'tp')
- wv_b: bfloat16 [5120, 1024], P(None, 'tp')
- k_norm: bfloat16 [128], replicated
- wo_b: bfloat16 [4096, 5120], P('tp')
- ln2_b: bfloat16 [5120], replicated
- wg_b: bfloat16 [5120, 14336], P(None, 'tp')
- wu_b: bfloat16 [5120, 14336], P(None, 'tp')
- wd_b: bfloat16 [14336, 5120], P('tp')
- xgates: float32 [2], replicated
Outputs:
- output: bfloat16 [8, 512, 5120], P('dp', 'tp'), parts along dimension 0
There are 4 independent parts. The reference program is written for one: setup_inputs(seed, part) draws one part's arguments, and reference() takes and returns one part's arrays. A program takes and returns all parts, laid end to end along the dimension named above; an argument that names none is the same for every part.
All inputs are finite; a program needn't handle non-finite values.
Results may differ from the reference program's by a relative error of at most 0.0167068.
Values are sent between devices in bfloat16 or wider.
A program may use at most 768 MiB of HBM per device.

```python
import math
import jax
import jax.numpy as jnp
from jax import lax

SAMPLES = 2
TOKENS = 512
VISION_TOKENS = 2048
MODEL_DIM = 5120
NUM_HEADS = 32
KV_HEADS = 8
HEAD_DIM = 128
FFN_DIM = 14336
NUM_TILES = 4

ROPE_THETA = 500000.0
ROPE_FACTOR = 8.0
LOW_FACTOR = 1.0
HIGH_FACTOR = 4.0
ORIG_CONTEXT = 8192.0
NORM_EPS = 1e-5
MASK_VALUE = -1e30


def rope_table(head_dim):
    low_wave = ORIG_CONTEXT / LOW_FACTOR
    high_wave = ORIG_CONTEXT / HIGH_FACTOR
    freq_list = []
    for freq_idx in range(head_dim // 2):
        base_freq = 1.0 / (ROPE_THETA ** (2.0 * freq_idx / head_dim))
        wave_len = 2.0 * math.pi / base_freq
        if wave_len > low_wave:
            freq_list.append(base_freq / ROPE_FACTOR)
        elif wave_len < high_wave:
            freq_list.append(base_freq)
        else:
            smooth = (ORIG_CONTEXT / wave_len - LOW_FACTOR) / (HIGH_FACTOR - LOW_FACTOR)
            freq_list.append((1.0 - smooth) * base_freq / ROPE_FACTOR + smooth * base_freq)
    return jnp.array(freq_list, dtype=jnp.float32)


def rms_scale(values, norm_gain):
    values = values.astype(jnp.float32)
    mean_sq = jnp.mean(values * values, axis=-1, keepdims=True)
    return values * lax.rsqrt(mean_sq + NORM_EPS) * norm_gain.astype(jnp.float32)


def rotate(values, cos_tab, sin_tab):
    half_dim = values.shape[-1] // 2
    first_half = values[..., :half_dim]
    second_half = values[..., half_dim:]
    return jnp.concatenate([first_half * cos_tab - second_half * sin_tab, second_half * cos_tab + first_half * sin_tab], axis=-1)


def group_attention(queries, key_vecs, val_vecs, allowed):
    def one_group(operands):
        query_grp, key_grp, val_grp = operands
        scores = jnp.einsum('rqd,kd->rqk', query_grp.astype(jnp.float32), key_grp.astype(jnp.float32)) * (HEAD_DIM ** -0.5)
        weights = jax.nn.softmax(jnp.where(allowed[None], scores, MASK_VALUE), axis=-1).astype(jnp.bfloat16)
        return jnp.einsum('rqk,kd->rqd', weights.astype(jnp.float32), val_grp.astype(jnp.float32)).astype(jnp.bfloat16)
    grouped = lax.map(one_group, (jnp.transpose(queries, (1, 2, 0, 3)), jnp.transpose(key_vecs, (1, 0, 2)), jnp.transpose(val_vecs, (1, 0, 2))))
    return jnp.transpose(grouped, (2, 0, 1, 3)).reshape(queries.shape[0], -1)


def gated_mlp(resid, norm_gain, w_gate, w_up, w_down):
    normed = rms_scale(resid, norm_gain).astype(jnp.bfloat16)
    gate_proj = jnp.dot(normed, w_gate, preferred_element_type=jnp.float32)
    up_proj = jnp.dot(normed, w_up, preferred_element_type=jnp.float32)
    activated = (jax.nn.silu(gate_proj) * up_proj).astype(jnp.bfloat16)
    return jnp.dot(activated, w_down, preferred_element_type=jnp.float32)


def setup_inputs(seed: int = 0, part: int = 0) -> dict:
    data_keys = jax.random.split(jax.random.fold_in(jax.random.key(seed + 1), part), 6)
    weight_keys = jax.random.split(jax.random.key(seed), 22)
    qk_scale = max(math.log(TOKENS / 8.0), 1.0) ** 0.25
    cross_gain = max(math.log(VISION_TOKENS / 16.0), 1.0) ** 0.25
    q_width = NUM_HEADS * HEAD_DIM
    kv_width = KV_HEADS * HEAD_DIM
    dim_scale = MODEL_DIM ** -0.5

    def draw_normal(key_val, arr_shape, spread):
        return (jax.random.normal(key_val, arr_shape, jnp.float32) * spread).astype(jnp.bfloat16)

    def draw_gain(key_val, arr_shape, center):
        return (center * (1.0 + 0.2 * jax.random.normal(key_val, arr_shape, jnp.float32))).astype(jnp.bfloat16)

    hidden = draw_normal(data_keys[0], (SAMPLES, TOKENS, MODEL_DIM), 1.0)
    vision = draw_normal(data_keys[1], (SAMPLES, VISION_TOKENS, MODEL_DIM), 1.0)
    pos_steps = jax.random.randint(data_keys[2], (SAMPLES, TOKENS), 1, 4, dtype=jnp.int32)
    offsets = jax.random.randint(data_keys[3], (SAMPLES, 1), 0, TOKENS, dtype=jnp.int32)
    positions = (offsets + jnp.cumsum(pos_steps, axis=1)).astype(jnp.int32)
    begins = jax.random.randint(data_keys[4], (SAMPLES, 1, 1), 0, TOKENS // 4 + 1, dtype=jnp.int32)
    tile_bits = jax.random.randint(data_keys[5], (SAMPLES, TOKENS, NUM_TILES), 0, 2, dtype=jnp.int32)
    tile_mask = jnp.where(jnp.arange(TOKENS, dtype=jnp.int32)[None, :, None] >= begins, tile_bits, 0).astype(jnp.int32)
    magnitudes = jax.random.uniform(weight_keys[20], (2,), jnp.float32, 0.6, 1.4)
    gate_signs = (2 * jax.random.randint(weight_keys[21], (2,), 0, 2, dtype=jnp.int32) - 1).astype(jnp.float32)
    return {
        'hidden': hidden,
        'vision': vision,
        'positions': positions,
        'tile_mask': tile_mask,
        'ln1_a': draw_gain(weight_keys[0], (MODEL_DIM,), 1.0),
        'wq_a': draw_normal(weight_keys[1], (MODEL_DIM, q_width), qk_scale * dim_scale),
        'wk_a': draw_normal(weight_keys[2], (MODEL_DIM, kv_width), qk_scale * dim_scale),
        'wv_a': draw_normal(weight_keys[3], (MODEL_DIM, kv_width), dim_scale),
        'wo_a': draw_normal(weight_keys[4], (q_width, MODEL_DIM), q_width ** -0.5),
        'ln2_a': draw_gain(weight_keys[5], (MODEL_DIM,), 1.0),
        'wg_a': draw_normal(weight_keys[6], (MODEL_DIM, FFN_DIM), dim_scale),
        'wu_a': draw_normal(weight_keys[7], (MODEL_DIM, FFN_DIM), dim_scale),
        'wd_a': draw_normal(weight_keys[8], (FFN_DIM, MODEL_DIM), FFN_DIM ** -0.5),
        'ln1_b': draw_gain(weight_keys[9], (MODEL_DIM,), 1.0),
        'wq_b': draw_normal(weight_keys[10], (MODEL_DIM, q_width), dim_scale),
        'q_norm': draw_gain(weight_keys[11], (HEAD_DIM,), cross_gain),
        'wk_b': draw_normal(weight_keys[12], (MODEL_DIM, kv_width), dim_scale),
        'wv_b': draw_normal(weight_keys[13], (MODEL_DIM, kv_width), dim_scale),
        'k_norm': draw_gain(weight_keys[14], (HEAD_DIM,), cross_gain),
        'wo_b': draw_normal(weight_keys[15], (q_width, MODEL_DIM), q_width ** -0.5),
        'ln2_b': draw_gain(weight_keys[16], (MODEL_DIM,), 1.0),
        'wg_b': draw_normal(weight_keys[17], (MODEL_DIM, FFN_DIM), dim_scale),
        'wu_b': draw_normal(weight_keys[18], (MODEL_DIM, FFN_DIM), dim_scale),
        'wd_b': draw_normal(weight_keys[19], (FFN_DIM, MODEL_DIM), FFN_DIM ** -0.5),
        'xgates': magnitudes * gate_signs,
    }


def reference(hidden, vision, positions, tile_mask, ln1_a, wq_a, wk_a, wv_a, wo_a, ln2_a, wg_a, wu_a, wd_a, ln1_b, wq_b, q_norm, wk_b, wv_b, k_norm, wo_b, ln2_b, wg_b, wu_b, wd_b, xgates):
    rep_heads = NUM_HEADS // KV_HEADS
    tile_len = VISION_TOKENS // NUM_TILES
    inv_freq = rope_table(HEAD_DIM)
    gate_vals = jnp.tanh(xgates.astype(jnp.float32))
    causal = lax.broadcasted_iota(jnp.int32, (TOKENS, TOKENS), 0) >= lax.broadcasted_iota(jnp.int32, (TOKENS, TOKENS), 1)

    def one_sample(operands):
        hid_rows, vis_rows, pos_row, mask_row = operands
        angles = pos_row.astype(jnp.float32)[:, None] * inv_freq[None, :]
        cos_tab = jnp.cos(angles)[:, None, :]
        sin_tab = jnp.sin(angles)[:, None, :]
        normed = rms_scale(hid_rows, ln1_a).astype(jnp.bfloat16)
        queries = jnp.dot(normed, wq_a, preferred_element_type=jnp.float32).reshape(TOKENS, NUM_HEADS, HEAD_DIM)
        queries = rotate(queries, cos_tab, sin_tab).astype(jnp.bfloat16).reshape(TOKENS, KV_HEADS, rep_heads, HEAD_DIM)
        key_vecs = jnp.dot(normed, wk_a, preferred_element_type=jnp.float32).reshape(TOKENS, KV_HEADS, HEAD_DIM)
        key_vecs = rotate(key_vecs, cos_tab, sin_tab).astype(jnp.bfloat16)
        val_vecs = jnp.dot(normed, wv_a, preferred_element_type=jnp.float32).astype(jnp.bfloat16).reshape(TOKENS, KV_HEADS, HEAD_DIM)
        context = group_attention(queries, key_vecs, val_vecs, causal)
        h_one = (hid_rows.astype(jnp.float32) + jnp.dot(context, wo_a, preferred_element_type=jnp.float32)).astype(jnp.bfloat16)
        h_two = (h_one.astype(jnp.float32) + gated_mlp(h_one, ln2_a, wg_a, wu_a, wd_a)).astype(jnp.bfloat16)
        normed = rms_scale(h_two, ln1_b).astype(jnp.bfloat16)
        queries = jnp.dot(normed, wq_b, preferred_element_type=jnp.float32).reshape(TOKENS, NUM_HEADS, HEAD_DIM)
        queries = rms_scale(queries, q_norm).astype(jnp.bfloat16).reshape(TOKENS, KV_HEADS, rep_heads, HEAD_DIM)
        key_vecs = jnp.dot(vis_rows, wk_b, preferred_element_type=jnp.float32).reshape(VISION_TOKENS, KV_HEADS, HEAD_DIM)
        key_vecs = rms_scale(key_vecs, k_norm).astype(jnp.bfloat16)
        val_vecs = jnp.dot(vis_rows, wv_b, preferred_element_type=jnp.float32).astype(jnp.bfloat16).reshape(VISION_TOKENS, KV_HEADS, HEAD_DIM)
        visible = mask_row > 0
        allowed = jnp.repeat(visible, tile_len, axis=1)
        context = group_attention(queries, key_vecs, val_vecs, allowed)
        row_keep = jnp.any(visible, axis=-1, keepdims=True).astype(jnp.float32)
        attn_out = jnp.dot(context, wo_b, preferred_element_type=jnp.float32)
        h_three = (h_two.astype(jnp.float32) + gate_vals[0] * row_keep * attn_out).astype(jnp.bfloat16)
        mlp_out = gated_mlp(h_three, ln2_b, wg_b, wu_b, wd_b)
        return (h_three.astype(jnp.float32) + gate_vals[1] * row_keep * mlp_out).astype(jnp.bfloat16)

    return lax.map(one_sample, (hidden, vision, positions, tile_mask))
```

```python
import functools
import math
import jax
import jax.numpy as jnp
from jax import lax
from jax.experimental import pallas as pl
from jax.experimental.pallas import tpu as pltpu
from jax.sharding import PartitionSpec as P

ROPE_THETA = 500000.0
ROPE_FACTOR = 8.0
LOW_FACTOR = 1.0
HIGH_FACTOR = 4.0
ORIG_CONTEXT = 8192.0
NORM_EPS = 1e-5
MASK_VALUE = -1e30
BF16 = jnp.bfloat16
F32 = jnp.float32
MESH = pl.DeviceIdType.MESH
LANES = 128
ROWS = 16


def rope_table(head_dim):
    low_wave = ORIG_CONTEXT / LOW_FACTOR
    high_wave = ORIG_CONTEXT / HIGH_FACTOR
    freq_list = []
    for freq_idx in range(head_dim // 2):
        base_freq = 1.0 / (ROPE_THETA ** (2.0 * freq_idx / head_dim))
        wave_len = 2.0 * math.pi / base_freq
        if wave_len > low_wave:
            freq_list.append(base_freq / ROPE_FACTOR)
        elif wave_len < high_wave:
            freq_list.append(base_freq)
        else:
            smooth = (ORIG_CONTEXT / wave_len - LOW_FACTOR) / (HIGH_FACTOR - LOW_FACTOR)
            freq_list.append((1.0 - smooth) * base_freq / ROPE_FACTOR + smooth * base_freq)
    return jnp.array(freq_list, dtype=F32)


def dot(a, b):
    return jnp.dot(a, b, preferred_element_type=F32)


def dot_t(a, b):
    return lax.dot_general(a, b, (((1,), (1,)), ((), ())), preferred_element_type=F32)


def head_norm(v, gain):
    return v * lax.rsqrt(jnp.mean(v * v, axis=-1, keepdims=True) + NORM_EPS) * gain


def kernel(cfg, hid, vis, tab, xgates, ln1_a, ln2_a, ln1_b, ln2_b, q_norm, k_norm, wq_a, wk_a, wv_a, wo_a, wg_a, wu_a, wd_a, wq_b, wk_b, wv_b, wo_b, wg_b, wu_b, wd_b,
           out, wk3, wv3, vsib,
           xg, pt, rb0, rb1, rb2, wt, dw, act, kvb, kvs, vt, tabg, hs,
           ssem, rsem, wsem, dsem, vtsem, tss, trs, fss, frs, vss, vrs, kss, krs, hsem, osem):
    tp, tl, dim, ffn, vl, heads, tiles, nt, dn, vm = cfg
    chips = tp // 2
    tokens = tp * tl
    half = dim // 2
    hd = LANES
    me = lax.axis_index('tp')
    core = lax.rem(me, 2)
    chip = me // 2
    sib = me + 1 - 2 * core
    right = lax.rem(me + 2, tp)
    left = lax.rem(me + tp - 2, tp)
    opp = lax.rem(me + 4, tp)
    sib_right, sib_left, sib_opp = (lax.rem(sib + d, tp) for d in (2, tp - 2, 4))
    scale = hd ** -0.5

    def rows(blk):
        return pl.ds(pl.multiple_of(blk * tl, tl), tl)

    def span(i, n):
        return pl.ds(pl.multiple_of(i * n, n), n)

    LO, HI, ALL = pl.ds(0, half), pl.ds(half, half), pl.ds(0, dim)

    def rdma(src, dst, ss, rs, dev):
        return pltpu.make_async_remote_copy(src_ref=src, dst_ref=dst, send_sem=ss, recv_sem=rs, device_id={'tp': dev}, device_id_type=MESH)

    def cp(s, i):
        xb = {0: chip, 1: lax.rem(chip + 1, chips), 2: lax.rem(chip + 2, chips), 3: lax.rem(chip + 3, chips)}
        sem = (ssem.at[s, i], rsem.at[s, i])
        if i < 4:
            b = 2 * xb[i] + 1 - core
            return rdma(pt.at[s, rows(b)], rb0.at[s, xb[i]], *sem, sib)
        if i == 4:
            return rdma(pt.at[s, rows(opp), LO], rb1.at[s, 0], *sem, right)
        if i == 5:
            return rdma(pt.at[s, rows(opp), HI], rb1.at[s, 1], *sem, left)
        if i == 6:
            return rdma(pt.at[s, rows(right), HI], rb2.at[s, 0, :, HI], *sem, right)
        if i == 7:
            return rdma(pt.at[s, rows(left), LO], rb2.at[s, 1, :, LO], *sem, left)
        if i == 8:
            return rdma(pt.at[s, rows(right), LO], rb2.at[s, 0, :, LO], *sem, right)
        if i == 9:
            return rdma(pt.at[s, rows(left), HI], rb2.at[s, 1, :, HI], *sem, left)

        def fwd(blk, cols, dev):
            ref = xg.at[s, rows(blk), cols]
            return rdma(ref, ref, *sem, dev)
        return {10: lambda: fwd(me, ALL, right), 11: lambda: fwd(me, ALL, left), 12: lambda: fwd(me, ALL, sib),
                13: lambda: fwd(left, LO, right), 14: lambda: fwd(right, HI, left),
                15: lambda: fwd(left, ALL, sib), 16: lambda: fwd(right, ALL, sib),
                17: lambda: fwd(opp, LO, sib), 18: lambda: fwd(opp, HI, sib)}[i]()

    def landed(s, i):
        sem = (ssem.at[s, i], rsem.at[s, i])
        if i < 10:
            return cp(s, i)
        blk, cols = {10: (left, ALL), 11: (right, ALL), 12: (sib, ALL), 13: (opp, LO), 14: (opp, HI),
                     15: (sib_left, ALL), 16: (sib_right, ALL), 17: (sib_opp, LO), 18: (sib_opp, HI)}[i]
        ref = xg.at[s, rows(blk), cols]
        return rdma(ref, ref, *sem, sib)

    def start(s, *ids):
        for i in ids:
            cp(s, i).start()

    def arrived(s, *ids):
        for i in ids:
            landed(s, i).wait_recv()

    def sent(s, *ids):
        for i in ids:
            cp(s, i).wait_send()

    def add_into(s, blk, cols, other):
        def body(r, _):
            at = pl.ds(pl.multiple_of(blk * tl + r * ROWS, ROWS), ROWS)
            src = pl.ds(pl.multiple_of(r * ROWS, ROWS), ROWS)
            pt[s, at, cols] = (pt[s, at, cols].astype(F32) + other(src).astype(F32)).astype(BF16)
            return 0
        lax.fori_loop(0, tl // ROWS, body, 0)

    def e0(s):
        start(s, 2, 1, 3, 0)

    def e1(s):
        for i, d in ((2, opp), (1, right), (3, left)):
            arrived(s, i)
            xb = d // 2
            add_into(s, d, ALL, lambda at, xb=xb: rb0[s, xb, at, :])
            if i == 1:
                start(s, 4, 5, 6)
        start(s, 7)

    def e2(s):
        arrived(s, 4)
        add_into(s, right, LO, lambda at: rb1[s, 0, at, :])
        arrived(s, 5)
        start(s, 8)
        add_into(s, left, HI, lambda at: rb1[s, 1, at, :])
        start(s, 9)

    def final(s, ln, gate, reduce, norm):
        gain = (ln1_a, ln2_a, ln1_b, ln2_b)[ln]

        def body(r, _):
            at = pl.ds(pl.multiple_of(r * ROWS, ROWS), ROWS)
            h = hs[s, at, :].astype(F32)
            if reduce:
                y = pt[s, pl.ds(pl.multiple_of(me * tl + r * ROWS, ROWS), ROWS), :].astype(F32) + rb0[s, chip, at, :].astype(F32)
                y = y + rb2[s, 0, at, :].astype(F32) + rb2[s, 1, at, :].astype(F32)
                if gate is not None:
                    keep = jnp.max(tab[2, at, s * tiles:(s + 1) * tiles], axis=-1, keepdims=True)
                    y = y * (jnp.tanh(xgates[0:1, gate:gate + 1]) * keep)
                hb = (h + y).astype(BF16)
                hs[s, at, :] = hb
                h = hb.astype(F32)
            if norm:
                x = h * lax.rsqrt(jnp.mean(h * h, axis=-1, keepdims=True) + NORM_EPS) * gain[...].astype(F32)
                xg[s, pl.ds(pl.multiple_of(me * tl + r * ROWS, ROWS), ROWS), :] = x.astype(BF16)
            return 0
        lax.fori_loop(0, tl // ROWS, body, 0)

    def e3(s, ln, gate=None, reduce=True, norm=True):
        if reduce:
            arrived(s, 0, 6, 7, 8, 9)
        final(s, ln, gate, reduce, norm)
        if norm:
            start(s, 10, 11, 12)

    def e4(s):
        arrived(s, 10)
        start(s, 13, 15)
        arrived(s, 11)
        start(s, 14, 16)

    def e5(s):
        arrived(s, 13)
        start(s, 17)
        arrived(s, 14)
        start(s, 18)

    def e6(s, reduce=True):
        arrived(s, 12, 15, 16, 17, 18)
        sent(s, *(range(19) if reduce else range(10, 19)))

    quarters = 4
    qr = dim // quarters
    cw = LANES

    def fcopy(kind, q, part, way):
        r = pl.ds(q * qr, qr)
        if kind == 'a':
            src = (wk_b, wv_b)[part].at[r]
            dst = (wk3, wv3)[part].at[1 if way else 0, r]
            i = (2 * q + part) + 8 * way
        else:
            arr = (wk3, wv3)[way]
            src = arr.at[way, r]
            dst = arr.at[2, r]
            i = 16 + q + 4 * way
        return rdma(src, dst, fss.at[i], frs.at[i], left if way else right)

    fill_list = [('a', q, part) for q in range(quarters) for part in range(2)] + [('b', q, None) for q in range(quarters)]
    fill_pos = [0]

    def fill(n):
        for _ in range(n):
            kind, q, part = fill_list[fill_pos[0]]
            fill_pos[0] += 1
            for way in (0, 1):
                if kind == 'b':
                    fcopy('a', q, way, way).wait_recv()
                    fcopy('b', q, None, way).start()
                else:
                    fcopy('a', q, part, way).start()

    def fill_done():
        for q in range(quarters):
            for way in (0, 1):
                fcopy('b', q, None, way).wait()
                fcopy('a', q, 0, way).wait_send()
                fcopy('a', q, 1, way).wait_send()
                fcopy('a', q, 1 - way, way).wait_recv()

    def wcopy(src, slot, cols=None):
        return pltpu.make_async_copy(src, wt.at[slot] if cols is None else wt.at[slot, :, cols], wsem.at[slot])

    def pairs(w, i, slot):
        return pltpu.make_async_copy(w.at[:, span(i, nt)], wt.at[slot], wsem.at[slot])

    def pf_mlp(wg, wu):
        pairs(wg, 0, 0).start()
        pairs(wu, 0, 1).start()

    def q_tiles(wq):
        return [pltpu.make_async_copy(wq.at[:, pl.ds(i * nt, nt)], wt.at[i], wsem.at[i]) for i in range(heads * hd // nt)]

    def kv_pair(k, v, slot):
        return [pltpu.make_async_copy(k, wt.at[slot, :, pl.ds(0, cw)], wsem.at[slot]), pltpu.make_async_copy(v, wt.at[slot, :, pl.ds(cw, cw)], vtsem.at[2 + slot])]

    def pf_self():
        for c in q_tiles(wq_a) + kv_pair(wk_a, wv_a, 2):
            c.start()

    def pf_cross():
        for c in q_tiles(wq_b):
            c.start()

    def run(events, i, j):
        for at, fs in events.items():
            @pl.when(j == at)
            def _():
                for f in fs:
                    f()

    def events_for(spec, n):
        got = {}
        for at, f in spec:
            got.setdefault(min(at, n - 1), []).append(f)
        return got

    def out_proj(s, w, depth, spec):
        nd = dim // dn
        events = events_for(spec, nd)

        def dcopy(n, slot):
            return pltpu.make_async_copy(w.at[:, span(n, dn)], dw.at[slot, pl.ds(0, depth)], dsem.at[slot])

        def body(n, _):
            slot = lax.rem(n, 2)

            @pl.when(n + 1 < nd)
            def _():
                dcopy(n + 1, 1 - slot).start()
            dcopy(n, slot).wait()
            pt[s, :, span(n, dn)] = dot(act[:, 0:depth], dw[slot, 0:depth, :]).astype(BF16)
            run(events, 0, n)
            return 0
        return (lambda: dcopy(0, 0).start()), (lambda: lax.fori_loop(0, nd, body, 0))

    def mlp(s, wg, wu, wd, spec_g, spec_d, prefetch):
        ng = ffn // nt
        events = events_for(spec_g, ng)
        first, project = out_proj(s, wd, ffn, spec_d)
        first()

        def body(j, _):
            slot = 2 * lax.rem(j, 2)
            other = 2 - slot

            @pl.when(j + 1 < ng)
            def _():
                pairs(wg, j + 1, other).start()
                pairs(wu, j + 1, other + 1).start()
            pairs(wg, j, slot).wait()
            pairs(wu, j, slot + 1).wait()
            x = xg[s]
            g = dot(x, wt[slot])
            u = dot(x, wt[slot + 1])
            act[:, span(j, nt)] = (g * jax.nn.sigmoid(g) * u).astype(BF16)
            run(events, 0, j)
            return 0
        lax.fori_loop(0, ng, body, 0)
        prefetch()
        project()

    QC, KC, VC = heads * hd, 2 * heads * hd, 2 * heads * hd + hd

    def self_part(s, spec_a, spec_d, prefetch):
        first, project = out_proj(s, wo_a, heads * hd, spec_d)
        first()
        t = tabg[:, s].reshape(tokens, LANES)
        lo = lax.broadcasted_iota(jnp.int32, (tokens, LANES), 1) < hd // 2
        tr = pltpu.roll(t, hd // 2, 1)
        cos = jnp.where(lo, t, tr)
        sin = jnp.where(lo, -tr, t)

        def rope(v):
            return (v * cos + pltpu.roll(v, hd // 2, 1) * sin).astype(BF16)
        x = xg[s]
        for i, c in enumerate(q_tiles(wq_a)):
            c.wait()
            q = dot(x, wt[i])
            for h in range(nt // hd):
                col = QC + i * nt + h * hd
                act[:, col:col + hd] = rope(q[:, h * hd:(h + 1) * hd])
        for c in kv_pair(wk_a, wv_a, 2):
            c.wait()
        kv = dot(x, wt[2])
        act[:, KC:KC + hd] = rope(kv[:, :hd])
        act[:, VC:VC + hd] = kv[:, hd:2 * hd].astype(BF16)
        prefetch()
        events = events_for(spec_a, heads)
        rb = min(256, tokens)

        def body(h, _):
            def blk(m, _):
                q = act[span(m, rb), pl.ds(pl.multiple_of(QC + h * hd, hd), hd)]
                sc = dot_t(q, act[:, KC:KC + hd]) * scale
                ok = lax.broadcasted_iota(jnp.int32, (rb, tokens), 0) + m * rb >= lax.broadcasted_iota(jnp.int32, (rb, tokens), 1)
                sc = jnp.where(ok, sc, MASK_VALUE)
                p = jnp.exp(sc - jnp.max(sc, axis=-1, keepdims=True))
                p = (p / jnp.sum(p, axis=-1, keepdims=True)).astype(BF16)
                act[span(m, rb), pl.ds(pl.multiple_of(h * hd, hd), hd)] = dot(p, act[:, VC:VC + hd]).astype(BF16)
                return 0
            lax.fori_loop(0, tokens // rb, blk, 0)
            run(events, 0, h)
            return 0
        lax.fori_loop(0, heads, body, 0)
        project()

    def cross_part(s, spec_a, spec_d, prefetch, kv_ready):
        first, project = out_proj(s, wo_b, heads * hd, spec_d)
        first()
        x = xg[s]
        for i, c in enumerate(q_tiles(wq_b)):
            c.wait()
            q = dot(x, wt[i])
            for h in range(nt // hd):
                col = QC + i * nt + h * hd
                act[:, col:col + hd] = head_norm(q[:, h * hd:(h + 1) * hd], q_norm[...].astype(F32)).astype(BF16)
        prefetch()
        kv_ready()
        rb = 2 * tl
        nb = tokens // rb
        events = events_for(spec_a, heads)

        def body(h, _):
            def blk(m, _):
                q = act[span(m, rb), pl.ds(pl.multiple_of(QC + h * hd, hd), hd)]
                seen = tabg[span(m, 2), 2].reshape(rb, LANES)
                sc = [jnp.where(seen[:, s * tiles + j:s * tiles + j + 1] > 0.5, dot_t(q, kvb[j, s, :, 0:hd]) * scale, MASK_VALUE) for j in range(tiles)]
                top = functools.reduce(jnp.maximum, [jnp.max(c, axis=-1, keepdims=True) for c in sc])
                ex = [jnp.exp(c - top) for c in sc]
                inv = 1.0 / functools.reduce(jnp.add, [jnp.sum(c, axis=-1, keepdims=True) for c in ex])
                o = functools.reduce(jnp.add, [dot((c * inv).astype(BF16), kvb[j, s, :, hd:2 * hd]) for j, c in enumerate(ex)])
                act[span(m, rb), pl.ds(pl.multiple_of(h * hd, hd), hd)] = o.astype(BF16)
                return 0
            lax.fori_loop(0, nb, blk, 0)
            run(events, 0, h)
            return 0
        lax.fori_loop(0, heads, body, 0)
        project()

    def kcopy(i):
        return rdma(kvs.at[i], kvb.at[chip], kss.at[i], krs.at[i], (left, right, opp)[i])

    def klanded(i):
        src = lax.rem(chip + (1, chips - 1, 2)[i], chips)
        return rdma(kvs.at[i], kvb.at[src], kss.at[i], krs.at[i], sib)

    def vcopy():
        return rdma(vis, vsib, vss, vrs, sib)

    def vision_part(spec, prefetch):
        fill_done()
        loads = kv_pair(wk_b, wv_b, 0) + [c for i in range(3) for c in kv_pair(wk3.at[i], wv3.at[i], 1 + i)]
        for c in loads:
            c.start()
        per = vl // vm
        n = 4 * per
        events = events_for(spec, n)

        def vload(i, slot, go):
            src, s, b = i // (2 * per), lax.rem(i // per, 2), lax.rem(i, per)

            @pl.when(src == 0)
            def _():
                go(pltpu.make_async_copy(vis.at[s, span(b, vm)], vt.at[slot], vtsem.at[slot]))

            @pl.when(src == 1)
            def _():
                go(pltpu.make_async_copy(vsib.at[s, span(b, vm)], vt.at[slot], vtsem.at[slot]))
        vload(0, 0, lambda c: c.start())
        vcopy().wait()
        for c in loads:
            c.wait()

        def body(i, _):
            slot = lax.rem(i, 2)
            src, s, b = i // (2 * per), lax.rem(i // per, 2), lax.rem(i, per)

            @pl.when(i + 1 < n)
            def _():
                vload(i + 1, 1 - slot, lambda c: c.start())
            vload(i, slot, lambda c: c.wait())
            owner = core + src - 2 * core * src
            at = pl.ds(pl.multiple_of(owner * vl + b * vm, vm), vm)
            v = vt[slot]
            for j in range(4):
                kv = dot(v, wt[j])
                kv = jnp.concatenate([head_norm(kv[:, :hd], k_norm[...].astype(F32)), kv[:, hd:]], axis=1).astype(BF16)
                if j == 0:
                    kvb[chip, s, at, :] = kv
                else:
                    kvs[j - 1, s, at, :] = kv
            run(events, 0, i)
            return 0
        lax.fori_loop(0, n, body, 0)
        prefetch()
        for i in range(3):
            kcopy(i).start()

    def kv_wait():
        for i in range(3):
            klanded(i).wait_recv()
            kcopy(i).wait_send()

    def tcopy(d):
        return rdma(tab, tabg.at[me], tss.at[d - 1], trs.at[d - 1], lax.rem(me + d, tp))

    def tlanded(d):
        return rdma(tab, tabg.at[lax.rem(me + tp - d, tp)], tss.at[d - 1], trs.at[d - 1], sib)

    def nothing():
        pass

    loads = [pltpu.make_async_copy(hid.at[s], hs.at[s], hsem.at[s]) for s in (0, 1)]
    for c in loads:
        c.start()
    pf_self()
    barrier = pltpu.get_barrier_semaphore()
    for d in range(1, tp):
        pl.semaphore_signal(barrier, inc=1, device_id={'tp': lax.rem(me + d, tp)}, device_id_type=MESH)
    pl.semaphore_wait(barrier, tp - 1)

    loads[0].wait()
    e3(0, 0, reduce=False)
    loads[1].wait()
    final(1, 0, None, False, True)
    for d in range(1, tp):
        tcopy(d).start()
    e4(0)
    start(1, 10, 11, 12)
    vcopy().start()
    tabg[me] = tab[...]
    e5(0)
    fill(2)
    e6(0, reduce=False)
    for d in range(1, tp):
        tlanded(d).wait_recv()
        tcopy(d).wait_send()

    self_part(0, [(0, lambda: e4(1)), (2, lambda: e5(1)), (2, lambda: fill(2))], [], nothing)
    e0(0)
    e6(1, reduce=False)
    e1(0)
    pf_self()
    self_part(1, [(1, lambda: e2(0)), (1, lambda: fill(1))], [], lambda: pf_mlp(wg_a, wu_a))
    e0(1)
    e3(0, 1)
    e1(1)
    e4(0)
    fill(1)
    e2(1)
    e5(0)
    e6(0)
    mlp(0, wg_a, wu_a, wd_a, [(0, lambda: fill(2)), (3, lambda: e3(1, 1)), (4, lambda: fill(1))], [(4, lambda: e4(1)), (5, lambda: fill(2))], lambda: pf_mlp(wg_a, wu_a))
    e0(0)
    e5(1)
    e1(0)
    e6(1)
    mlp(1, wg_a, wu_a, wd_a, [(0, lambda: fill(1)), (1, lambda: e2(0)), (5, lambda: e3(0, 2))], [], nothing)
    e0(1)
    e4(0)
    e1(1)
    vision_part([(1, lambda: e2(1)), (3, lambda: e5(0))], pf_cross)
    e6(0)
    cross_part(0, [(1, lambda: e3(1, 2))], [(2, lambda: e4(1)), (8, lambda: e5(1))], pf_cross, kv_wait)
    e0(0)
    e1(0)
    e6(1)
    cross_part(1, [(1, lambda: e2(0))], [(4, lambda: e3(0, 3, gate=0))], lambda: pf_mlp(wg_b, wu_b), nothing)
    e0(1)
    e1(1)
    e4(0)
    e2(1)
    e5(0)
    e6(0)
    mlp(0, wg_b, wu_b, wd_b, [(3, lambda: e3(1, 3, gate=0))], [(4, lambda: e4(1))], lambda: pf_mlp(wg_b, wu_b))
    e0(0)
    e5(1)
    e1(0)
    e6(1)

    def ocopy(s):
        return pltpu.make_async_copy(hs.at[s], out.at[s], osem.at[s])

    def done(s):
        e3(s, 0, gate=1, norm=False)
        ocopy(s).start()
    mlp(1, wg_b, wu_b, wd_b, [(1, lambda: e2(0)), (5, lambda: done(0))], [], nothing)
    e0(1)
    e1(1)
    e2(1)
    done(1)
    for s in (0, 1):
        sent(s, *range(10))
        ocopy(s).wait()


def solution(mesh):
    act_spec = P('dp', 'tp', None)
    col_spec = P(None, 'tp')
    row_spec = P('tp', None)
    layer_a = (P(), col_spec, col_spec, col_spec, row_spec, P(), col_spec, col_spec, row_spec)
    layer_b = (P(), col_spec, P(), col_spec, col_spec, P(), row_spec, P(), col_spec, col_spec, row_spec, P())
    in_specs = (act_spec, act_spec, P('dp', 'tp'), act_spec) + layer_a + layer_b
    tp = mesh.shape['tp']

    def body(hidden, vision, positions, tile_mask, ln1_a, wq_a, wk_a, wv_a, wo_a, ln2_a, wg_a, wu_a, wd_a, ln1_b, wq_b, q_norm, wk_b, wv_b, k_norm, wo_b, ln2_b, wg_b, wu_b, wd_b, xgates):
        hd = q_norm.shape[0]
        samples, tl, dim = hidden.shape
        vl = vision.shape[1]
        tiles = tile_mask.shape[2]
        ffn = wg_a.shape[1]
        heads = wq_a.shape[1] // hd
        nt, dn, vm = 256, min(512, dim // 2), 128
        tokens, chips = tp * tl, tp // 2
        assert samples == 2 and tp == 8 and tiles == chips and hd == LANES and wk_a.shape[1] == hd
        cfg = (tp, tl, dim, ffn, vl, heads, tiles, nt, dn, vm)
        ang = positions.astype(F32)[..., None] * rope_table(hd)
        rope = jnp.concatenate([jnp.cos(ang), jnp.sin(ang)], axis=-1)
        seen = jnp.moveaxis(tile_mask, 0, 1).reshape(tl, samples * tiles).astype(F32)
        tab = jnp.concatenate([rope, jnp.pad(seen, ((0, 0), (0, LANES - samples * tiles)))[None]], axis=0)
        anyspec = pl.BlockSpec(memory_space=pl.ANY)
        vspec = pl.BlockSpec(memory_space=pltpu.VMEM)
        sds = jax.ShapeDtypeStruct
        dma = pltpu.SemaphoreType.DMA
        res = pl.pallas_call(
            functools.partial(kernel, cfg),
            out_shape=[sds((samples, tl, dim), BF16), sds((3, dim, hd), BF16), sds((3, dim, hd), BF16), sds((samples, vl, dim), BF16)],
            in_specs=[anyspec] * 2 + [vspec] * 8 + [anyspec] * 14,
            out_specs=[anyspec] * 4,
            scratch_shapes=[
                pltpu.VMEM((2, tokens, dim), BF16),
                pltpu.VMEM((2, tokens, dim), BF16),
                pltpu.VMEM((2, chips, tl, dim), BF16),
                pltpu.VMEM((2, 2, tl, dim // 2), BF16),
                pltpu.VMEM((2, 2, tl, dim), BF16),
                pltpu.VMEM((4, dim, nt), BF16),
                pltpu.VMEM((2, max(ffn, heads * hd), dn), BF16),
                pltpu.VMEM((tokens, max(ffn, (2 * heads + 2) * hd)), BF16),
                pltpu.VMEM((chips, 2, 2 * vl, 2 * hd), BF16),
                pltpu.VMEM((3, 2, 2 * vl, 2 * hd), BF16),
                pltpu.VMEM((2, vm, dim), BF16),
                pltpu.VMEM((tp, 3, tl, LANES), F32),
                pltpu.VMEM((2, tl, dim), BF16),
                dma((2, 19)), dma((2, 19)), dma((4,)), dma((2,)), dma((6,)), dma((7,)), dma((7,)), dma((24,)), dma((24,)), dma, dma, dma((3,)), dma((3,)), dma((2,)), dma((2,)),
            ],
            compiler_params=pltpu.CompilerParams(collective_id=0, has_side_effects=True, vmem_limit_bytes=67043328),
            name='layers',
        )(hidden, vision, tab, xgates.reshape(1, 2), *(g.reshape(1, -1) for g in (ln1_a, ln2_a, ln1_b, ln2_b, q_norm, k_norm)), wq_a, wk_a, wv_a, wo_a, wg_a, wu_a, wd_a, wq_b, wk_b, wv_b, wo_b, wg_b, wu_b, wd_b)
        return res[0]

    return jax.shard_map(body, mesh=mesh, in_specs=in_specs, out_specs=act_spec, check_vma=False)
```
